32 devices in a mesh: dp: 4 (over x, core), mp: 8 (over z, y).
Axes of the slice: x: 2, y: 2, z: 4, core: 2. Of those that a mesh axis runs over, the one named last changes fastest.
Arguments:
- cotangent: bfloat16 [512, 4608], P(('dp', 'mp')), may hold values from -50 to 50
- mlp_out: bfloat16 [512, 4608], P(('dp', 'mp')), may hold values from -500 to 500
- post_gain: float32 [4608], replicated, may hold values from 0.5 to 1.5
- down_weight: bfloat16 [36864, 4608], P('mp', 'dp'), may hold values from -0.09375 to 0.09375
- gate_pre: bfloat16 [512, 36864], P('dp', 'mp'), may hold values from -6 to 6
- up_pre: bfloat16 [512, 36864], P('dp', 'mp'), may hold values from -6 to 6
Outputs:
- gate_grad: float32 [512, 36864], P('dp', 'mp')
- up_grad: float32 [512, 36864], P('dp', 'mp')
- gain_grad: float32 [4608], replicated
The draws below stay inside these ranges and needn't reach their ends.
All inputs are finite; a program needn't handle non-finite values.
Results may differ from the reference program's by a relative error of at most 0.0005.
Values may be sent and summed in bfloat16 or wider, within the bound.
A program may use at most 64 MiB of HBM per device.

```python
import jax
import jax.numpy as jnp
from jax import lax

D = 4608
FF = 36864
TOKENS = 512


def draw_cotangent(key, part):
    noise_key, jitter_key = jax.random.split(jax.random.fold_in(key, 17))
    row_pos = jnp.arange(TOKENS, dtype=jnp.float32)[:, None] / TOKENS
    jitter = jax.random.uniform(jitter_key, (TOKENS, 1), jnp.float32)
    values = jnp.clip(jax.random.normal(noise_key, (TOKENS, D), jnp.float32), -5.0, 5.0)
    row_exp = 0.5 * row_pos + 0.5 * jitter
    return (values * 10.0 ** row_exp).astype(jnp.bfloat16)


def draw_mlp_out(key, part):
    noise_key, row_key, col_key = jax.random.split(jax.random.fold_in(key, 29), 3)
    row_exp = jax.random.uniform(row_key, (TOKENS, 1), jnp.float32)
    col_exp = jax.random.uniform(col_key, (1, D), jnp.float32)
    values = jnp.clip(jax.random.normal(noise_key, (TOKENS, D), jnp.float32), -5.0, 5.0)
    return (values * 10.0 ** row_exp * 10.0 ** col_exp).astype(jnp.bfloat16)


def steps_of(own_key, shape, cuts, smallest, top_value):
    loudness = 1.0
    for dim, parts in cuts:
        heights = jax.random.uniform(jax.random.fold_in(jax.random.fold_in(own_key, 6), dim), (parts,), jnp.float32, smallest / len(cuts), top_value / len(cuts))
        loudness = loudness * jnp.repeat(jnp.exp(heights), shape[dim] // parts).reshape((-1,) + (1,) * (len(shape) - 1 - dim))
    return loudness


def bell_draw(rng, shape, deviation, most, cuts=(), kind=jnp.bfloat16):
    values = jax.random.normal(rng, shape, jnp.float32) * deviation
    if len(cuts) > 0:
        values = steps_of(rng, shape, cuts, -0.22, 0.18) * values
    return jnp.clip(values, min=-most, max=most).astype(kind)


def setup_inputs(seed: int = 0) -> dict:
    arg_keys = jax.random.split(jax.random.key(seed), 7)
    cotangent = draw_cotangent(jax.random.fold_in(arg_keys[6], 71), 0)
    mlp_out = draw_mlp_out(jax.random.fold_in(arg_keys[6], 71), 0)
    post_gain = jnp.clip(1.0 + 0.1 * jax.random.normal(arg_keys[2], (D,), jnp.float32), 0.5, 1.5)
    down_weight = bell_draw(arg_keys[3], (FF, D), D ** -0.5, 0.09375, ((0, 8), (1, 4)))
    gate_pre = bell_draw(arg_keys[4], (TOKENS, FF), 1.0, 6.0, ((0, 4), (1, 8)))
    up_pre = bell_draw(arg_keys[5], (TOKENS, FF), 1.0, 6.0, ((0, 4), (1, 8)))
    return {"cotangent": cotangent, "mlp_out": mlp_out, "post_gain": post_gain, "down_weight": down_weight, "gate_pre": gate_pre, "up_pre": up_pre}


epsilon = 1e-06

def gelu_tanh(values):
    return jax.nn.gelu(values, approximate=True)

def reference(cotangent, mlp_out, post_gain, down_weight, gate_pre, up_pre):
    forward = mlp_out.astype(jnp.float32)
    upstream = cotangent.astype(jnp.float32)
    root_mean = jnp.sqrt(lax.optimization_barrier(jnp.mean(forward * forward, axis=1, keepdims=True)) + epsilon)
    normed = forward / root_mean
    gain_grad = lax.optimization_barrier(jnp.sum(upstream * normed, axis=0))
    scaled = upstream * post_gain[None, :]
    project_sum = lax.optimization_barrier(jnp.sum(scaled * forward, axis=1, keepdims=True))
    out_grad = scaled / root_mean - forward * project_sum / (D * root_mean ** 3)
    hidden_grad = jnp.dot(out_grad, down_weight.astype(jnp.float32).T, precision=lax.Precision.HIGHEST)
    gate_val = gate_pre.astype(jnp.float32)
    up_val = up_pre.astype(jnp.float32)
    act_val, pull_back = jax.vjp(gelu_tanh, gate_val)
    gate_grad = pull_back(hidden_grad * up_val)[0]
    up_grad = hidden_grad * act_val
    return (gate_grad, up_grad, gain_grad)
```

```python
import functools
import math

import jax
import jax.numpy as jnp
from jax import lax
from jax.experimental import pallas as pl
from jax.experimental.pallas import tpu as pltpu
from jax.sharding import PartitionSpec as P

MESH = pl.DeviceIdType.MESH
LANES = 128
WEIGHT_MAX = 0.09375

epsilon = 1e-06


def gelu_tanh(values):
    return jax.nn.gelu(values, approximate=True)


def encode(v):
    v2 = v * v
    v4 = v2 * v2
    return (v2 * v * v4 * jnp.abs(v)).astype(jnp.bfloat16)


def decode(codes):
    b = codes.astype(jnp.float32)
    size = jnp.abs(b)
    root = jnp.exp2(jnp.log2(size) * 0.125)
    root = jnp.where(size > 0, root, 0.0)
    return jnp.where(b < 0, -root, root)


def groups_of(mp):
    away = [(0, 1), (1, 1), (2, 1)]
    start = 3
    while start < mp:
        count = min(2, mp - start) if mp - start > 3 else mp - start
        away.append((start, count))
        start += count
    step = min(4, mp)
    home = [(q, step) for q in range(0, mp, step)]
    order = [(0, g) for g in range(len(away))] + [(1, g) for g in range(len(home))]
    return away, home, order


def kernel(
    dp, mp, gain, tile, wide,
    c_hbm, y_hbm, post_hbm, w_hbm, gate_hbm, up_hbm, gate_out, up_out, gain_out,
    c_ref, y_ref, post_ref, w_ref, wt_ref, gate_ref, up_ref,
    code, grad, size_ref, lhs, mine, dsend, drecv, xsend, got,
    gsend_a, grecv_a, gsum, grecv_b, gblock, gall,
    in_sem, w_sem, act_sem, a_send, a_recv, s_send, s_recv, ga_send, ga_recv, gb_send, gb_recv, go_send, go_recv,
    z_send, y_send, g_recv, d_send, d_recv, x_send, x_recv,
):
    d, m = lax.axis_index("dp"), lax.axis_index("mp")
    nz = mp // 2
    x, core = d // 2, lax.rem(d, 2)
    z, y = m // 2, lax.rem(m, 2)
    rows, full = c_ref.shape
    hid, feat = w_ref.shape
    tiles = hid // tile
    away, home, order = groups_of(mp)

    def remote(src, dst, send, recv, dev):
        return pltpu.make_async_remote_copy(
            src_ref=src, dst_ref=dst, send_sem=send, recv_sem=recv, device_id=dev, device_id_type=MESH
        )

    first = [
        pltpu.make_async_copy(y_hbm, y_ref, in_sem.at[0]),
        pltpu.make_async_copy(c_hbm, c_ref, in_sem.at[1]),
        pltpu.make_async_copy(post_hbm, post_ref, in_sem.at[2]),
    ]
    for copy in first:
        copy.start()

    def many(h, g):
        return 1 if (h, g) == (0, 0) else wide

    def slot(h, g):
        n = order.index((h, g))
        return sum(tiles // many(*one) for one in order[:n])

    def lag(h, g):
        return min(4, tiles) if many(h, g) == 1 else min(2, tiles // wide)

    def w_copy(i):
        units = pl.ds(pl.multiple_of(i * (wide * tile), wide * tile), wide * tile)
        return pltpu.make_async_copy(w_hbm.at[units, :], w_ref.at[units, :], w_sem.at[i])

    acts = [
        pltpu.make_async_copy(gate_hbm, gate_ref, act_sem.at[0]),
        pltpu.make_async_copy(up_hbm, up_ref, act_sem.at[1]),
    ]
    barrier = pltpu.get_barrier_semaphore()
    for j in range(1, dp):
        pl.semaphore_signal(barrier, inc=1, device_id=(lax.rem(d + j, dp), m), device_id_type=MESH)
    for j in range(1, mp):
        pl.semaphore_signal(barrier, inc=1, device_id=(d, lax.rem(m + j, mp)), device_id_type=MESH)

    for copy in first:
        copy.wait()
    for i in range(tiles // wide):
        w_copy(i).start()
    forward = y_ref[...].astype(jnp.float32)
    upstream = c_ref[...].astype(jnp.float32)
    inv = 1.0 / jnp.sqrt(jnp.mean(forward * forward, axis=1, keepdims=True) + epsilon)
    normed = forward * inv
    scaled = upstream * post_ref[...].reshape(1, full)
    mean_prod = jnp.sum(scaled * normed, axis=1, keepdims=True) * (1.0 / full)
    out_grad = (scaled - normed * mean_prod) * inv
    top = jnp.max(jnp.abs(out_grad), axis=1, keepdims=True)
    top = jnp.where(top > 1e-37, top, 1.0)
    codes = encode(out_grad * (gain / top))
    for t in range(dp):
        code[t] = codes[:, t * feat:(t + 1) * feat]
    grad[1, m, core] = code[d]
    size_ref[m] = jnp.broadcast_to(top * (1.0 / gain), (rows, LANES))

    pl.semaphore_wait(barrier, dp - 1 + mp - 1)

    def a_far(c):
        t = 2 * (1 - x) + c
        return remote(code.at[t], grad.at[0, m, core], a_send.at[c], a_recv.at[core], (t, m))

    def a_far_wait(c):
        t = 2 * (1 - x) + c
        return remote(code.at[t], grad.at[0, m, c], a_send.at[c], a_recv.at[c], (t, m))

    def a_near():
        t = 2 * x + 1 - core
        return remote(code.at[t], grad.at[1, m, core], a_send.at[2], a_recv.at[2], (t, m))

    for c in range(2):
        a_far(c).start()
    a_near().start()

    gain_part = jnp.sum(upstream * normed, axis=0, keepdims=True)
    for t in range(dp):
        gsend_a[t] = gain_part[:, t * feat:(t + 1) * feat]

    def ga_copy(j):
        t = lax.rem(d + j, dp)
        return remote(gsend_a.at[t], grecv_a.at[j], ga_send, ga_recv, (t, m))

    def ga_all():
        return remote(gsend_a.at[pl.ds(1, dp - 1)], grecv_a.at[pl.ds(1, dp - 1)], ga_send, ga_recv, (lax.rem(d + 1, dp), m))

    for j in range(1, dp):
        ga_copy(j).start()

    def turn_over(i, carry):
        units = pl.ds(pl.multiple_of(i * (wide * tile), wide * tile), wide * tile)
        w_copy(i).wait()
        wt_ref[:, units] = w_ref[units, :].T
        return carry

    lax.fori_loop(0, tiles // wide, turn_over, 0)
    for copy in acts:
        copy.start()

    def s_copy(j):
        return remote(size_ref.at[m], size_ref.at[m], s_send, s_recv, (d, lax.rem(m + j, mp)))

    def s_all():
        some = pl.ds(0, mp - 1)
        return remote(size_ref.at[some], size_ref.at[some], s_send, s_recv, (d, lax.rem(m + 1, mp)))

    def place_z(p):
        low = jnp.minimum(z, nz - 1 - z)
        odd = p % 2
        near = z + odd * ((p + 1) // 2) - (1 - odd) * (p // 2)
        up = jnp.where(2 * z < nz - 1, 1, -1)
        return jnp.where(p <= 2 * low, near, z + up * (p - low))

    def level(q):
        if q == 2:
            return 1, True
        if q == mp - 1:
            return nz - 1, False
        return ((q + 1) // 2, True) if q % 2 else ((q - 2) // 2, False)

    def place(q):
        if q == 0:
            return m
        if q == 1:
            return 2 * z + 1 - y
        p, same = level(q)
        return 2 * place_z(p) + (y if same else 1 - y)

    def z_copy(h, p):
        return remote(grad.at[h, m], grad.at[h, m], z_send, g_recv.at[h, m], (d, 2 * place_z(p) + y))

    def y_copy(h, p):
        mc = 2 * place_z(p) + y if p else m
        return remote(grad.at[h, mc], grad.at[h, mc], y_send, g_recv.at[h, mc], (d, 2 * z + 1 - y))

    def g_wait(h, q):
        mc = place(q)
        remote(grad.at[h, mc], grad.at[h, mc], y_send, g_recv.at[h, mc], (d, 2 * z + 1 - y)).wait_recv()

    def spread_z(h):
        for p in range(1, nz):
            z_copy(h, p).start()

    def d_copy(h, g, i):
        q, n = (away, home)[h][g]
        at, some = pl.ds(q * rows, n * rows), pl.ds(i * many(h, g), many(h, g))
        return remote(
            dsend.at[h, some, at, :], drecv.at[h, some, at, :], d_send, d_recv.at[slot(h, g) + i],
            (2 * x + 1 - core, m),
        )

    def x_copy(g, i):
        q, n = away[g]
        at, some = pl.ds(q * rows, n * rows), pl.ds(i * many(0, g), many(0, g))
        return remote(
            xsend.at[some, at, :], got.at[some, at, :], x_send, x_recv.at[slot(0, g) + i], (2 * (1 - x) + core, m)
        )

    def unpack(h, g):
        q0, n = (away, home)[h][g]
        base, span = 4 * q0 * rows, n * rows
        for k in range(n):
            mc = place(q0 + k)
            for s in range(2):
                value = decode(grad[h, mc, core if s == 0 else 1 - core])
                high = value.astype(jnp.bfloat16)
                at = base + s * span + k * rows
                lhs[h, at:at + rows, :] = high
                lhs[h, at + 2 * span:at + 2 * span + rows, :] = (value - high.astype(jnp.float32)).astype(jnp.bfloat16)

    def compute(h, g, i):
        q, n = (away, home)[h][g]
        base, span = 4 * q * rows, n * rows
        width = many(h, g) * tile
        units = pl.ds(pl.multiple_of(i * width, width), width)
        both = lax.dot_general(
            lhs[h, base:base + 4 * span, :], wt_ref[:, units], (((1,), (0,)), ((), ())),
            preferred_element_type=jnp.float32,
        )
        both = both[:2 * span] + both[2 * span:]
        for k in range(many(h, g)):
            cols = slice(k * tile, (k + 1) * tile)
            mine[h, i * many(h, g) + k, q * rows:q * rows + span, :] = both[:span, cols]
            dsend[h, i * many(h, g) + k, q * rows:q * rows + span, :] = both[span:, cols]
        d_copy(h, g, i).start()

    def reduce(h, g, i):
        d_copy(h, g, i).wait_recv()
        if h == 0:
            q, n = away[g]
            at = slice(q * rows, (q + n) * rows)
            for k in range(many(h, g)):
                t = i * many(h, g) + k
                xsend[t, at, :] = encode(mine[0, t, at, :] + drecv[0, t, at, :])
            x_copy(g, i).start()

    def steps(h, g):
        return tiles // many(h, g)

    def run(n):
        h, g = order[n]
        late = lag(h, g)
        left = lag(*order[n - 1]) if n > 1 else 0
        each = -(-left // steps(h, g))

        def one(i, carry):
            compute(h, g, i)
            for k in range(each):
                j = i * each + k

                @pl.when(j < left)
                def _():
                    reduce(*order[n - 1], steps(*order[n - 1]) - left + j)

            @pl.when(i >= late)
            def _():
                reduce(h, g, i - late)

            return carry

        lax.fori_loop(0, steps(h, g), one, 0)

    def flush(n):
        h, g = order[n]

        def one(i, carry):
            reduce(h, g, i)
            return carry

        lax.fori_loop(steps(h, g) - lag(h, g), steps(h, g), one, 0)

    waited = [{0}, {0}]

    def arrive(h, q):
        if q in waited[h]:
            return
        waited[h].add(q)
        g_wait(h, q)
        if q > 1 and level(q)[1]:
            y_copy(h, level(q)[0]).start()

    def ready(h, g):
        q0, n = (away, home)[h][g]
        for q in range(q0, q0 + n):
            arrive(h, q)
        unpack(h, g)

    for c in range(2):
        a_far_wait(c).wait_recv()
    y_copy(0, 0).start()
    spread_z(0)
    for j in range(1, mp):
        s_copy(j).start()

    def near_wait():
        remote(code.at[0], grad.at[1, m, 1 - core], a_send.at[2], a_recv.at[2], (2 * x + 1 - core, m)).wait_recv()

    def gb_copy(j):
        return remote(gsum, grecv_b.at[j], gb_send, gb_recv, (d, lax.rem(m + j, mp)))

    def gb_all():
        some = grecv_b.at[pl.ds(1, mp - 1)]
        return remote(some, some, gb_send, gb_recv, (d, lax.rem(m + 1, mp)))

    def go_copy(j):
        return remote(gblock, gall.at[d], go_send, go_recv, (lax.rem(d + j, dp), m))

    def go_all():
        some = gall.at[pl.ds(0, dp - 1)]
        return remote(some, some, go_send, go_recv, (lax.rem(d + 1, dp), m))

    for n in range(len(order)):
        if n == 3 or order[n] == (1, 0):
            for q in range(2, mp):
                if level(q)[1]:
                    arrive(order[n][0], q)
        ready(*order[n])
        run(n)
        if n == 0:
            flush(n)
            near_wait()
            y_copy(1, 0).start()
            ga_all().wait_recv()
            total = gsend_a[d]
            for j in range(1, dp):
                total = total + grecv_a[j]
            gsum[...] = total
            for j in range(1, mp):
                gb_copy(j).start()
        if n == 1:
            spread_z(1)
        if order[n] == (1, 0):
            gtotal = gsum[...]
            gb_all().wait()
            for j in range(1, mp):
                gtotal = gtotal + grecv_b[j]
            gblock[...] = gtotal
            gall[d] = gtotal
            for j in range(1, dp):
                go_copy(j).start()

    flush(len(order) - 1)

    s_all().wait_recv()
    for copy in acts:
        copy.wait()

    slope = math.sqrt(2.0 / math.pi)

    def finish(g):
        q0, n = away[g]

        def one(i, carry):
            x_copy(g, i).wait_recv()
            for k in range(many(0, g)):
                t = i * many(0, g) + k
                cols = pl.ds(pl.multiple_of(t * tile, tile), tile)
                for q in range(q0, q0 + n):
                    mc = place(q)
                    at = slice(q * rows, (q + 1) * rows)
                    value = mine[1, t, at, :] + drecv[1, t, at, :] + decode(got[t, at, :])
                    value = value * size_ref[mc][:, :1]
                    gate = gate_ref[mc, :, cols].astype(jnp.float32)
                    up = up_ref[mc, :, cols].astype(jnp.float32)
                    square = gate * gate
                    bent = jnp.tanh(gate * (slope + (slope * 0.044715) * square))
                    half = 0.5 + 0.5 * bent
                    up_out[mc, :, cols] = value * (gate * half)
                    turn = half + (0.5 * gate) * (1.0 - bent * bent) * (slope + (3.0 * slope * 0.044715) * square)
                    gate_out[mc, :, cols] = (value * up) * turn
            return carry

        lax.fori_loop(0, steps(0, g), one, 0)

    for g in range(len(away)):
        finish(g)

    go_all().wait()
    for t in range(dp):
        gain_out[t * feat:(t + 1) * feat] = gall[t].reshape(feat)

    a_far(0).wait_send()
    a_far(1).wait_send()
    a_near().wait_send()
    ga_all().wait_send()
    s_all().wait_send()
    remote(grad.at[0], grad.at[0], y_send, g_recv.at[0, m], (d, 2 * z + 1 - y)).wait_send()
    some = grad.at[0, pl.ds(0, 2 * (nz - 1))]
    remote(some, some, z_send, g_recv.at[0, m], (d, 2 * z + 1 - y)).wait_send()
    remote(dsend, drecv, d_send, d_recv.at[0], (2 * x + 1 - core, m)).wait_send()
    remote(xsend, got, x_send, x_recv.at[0], (2 * (1 - x) + core, m)).wait_send()


def store(gate_in, up_in, gain_in, gate_to, up_to, gain_to, sem):
    copies = [
        pltpu.make_async_copy(src, dst, sem.at[n])
        for n, (src, dst) in enumerate(((gate_in, gate_to), (up_in, up_to), (gain_in, gain_to)))
    ]
    for copy in copies:
        copy.start()
    for copy in copies:
        copy.wait()


def fused(dp, mp, cotangent, mlp_out, post_gain, down_weight, gate_pre, up_pre):
    rows, full = cotangent.shape
    hid, feat = down_weight.shape
    nz = mp // 2
    gain = 2.0 ** math.floor(15.8 - math.log2(full * WEIGHT_MAX))
    tile = tile_of(hid)
    tiles = hid // tile
    wide = next(k for k in (3, 2, 1) if tiles % k == 0)
    bf, f32 = jnp.bfloat16, jnp.float32
    dma = pltpu.SemaphoreType.DMA
    span = mp * rows
    steps = tiles + tiles // wide * (len(groups_of(mp)[2]) - 1)
    hbm_spec = pl.BlockSpec(memory_space=pltpu.HBM)
    vmem_spec = pl.BlockSpec(memory_space=pltpu.VMEM)
    gate_grad, up_grad, gain_grad = pl.pallas_call(
        functools.partial(kernel, dp, mp, gain, tile, wide),
        out_shape=(
            pltpu.VMEM((mp, rows, hid), f32),
            pltpu.VMEM((mp, rows, hid), f32),
            pltpu.VMEM((full,), f32),
        ),
        in_specs=[hbm_spec] * 6,
        out_specs=(vmem_spec,) * 3,
        scratch_shapes=[
            pltpu.VMEM((rows, full), bf),
            pltpu.VMEM((rows, full), bf),
            pltpu.VMEM((full,), f32),
            pltpu.VMEM((hid, feat), bf),
            pltpu.VMEM((feat, hid), bf),
            pltpu.VMEM((mp, rows, hid), bf),
            pltpu.VMEM((mp, rows, hid), bf),
            pltpu.VMEM((dp, rows, feat), bf),
            pltpu.VMEM((2, mp, 2, rows, feat), bf),
            pltpu.VMEM((mp, rows, LANES), f32),
            pltpu.VMEM((2, 4 * span, feat), bf),
            pltpu.VMEM((2, tiles, span, tile), f32),
            pltpu.VMEM((2, tiles, span, tile), f32),
            pltpu.VMEM((2, tiles, span, tile), f32),
            pltpu.VMEM((tiles, span, tile), bf),
            pltpu.VMEM((tiles, span, tile), bf),
            pltpu.VMEM((dp, 1, feat), f32),
            pltpu.VMEM((dp, 1, feat), f32),
            pltpu.VMEM((1, feat), f32),
            pltpu.VMEM((mp, 1, feat), f32),
            pltpu.VMEM((1, feat), f32),
            pltpu.VMEM((dp, 1, feat), f32),
            dma((3,)), dma((tiles // wide,)), dma((2,)), dma((3,)), dma((3,)), dma, dma,
            dma, dma, dma, dma, dma, dma,
            dma, dma, dma((2, mp)),
            dma, dma((steps,)), dma, dma((steps,)),
        ],
        compiler_params=pltpu.CompilerParams(
            collective_id=0, has_side_effects=True, vmem_limit_bytes=52 * 1024 * 1024
        ),
        name="norm_gather_project_reduce",
    )(*(
        pltpu.with_memory_space_constraint(value, pltpu.HBM)
        for value in (
            cotangent, mlp_out, post_gain, down_weight,
            gate_pre.reshape(mp, rows, hid), up_pre.reshape(mp, rows, hid),
        )
    ))
    outs = (gate_grad, up_grad, gain_grad)
    gate_grad, up_grad, gain_grad = pl.pallas_call(
        store,
        out_shape=tuple(pltpu.HBM(value.shape, f32) for value in outs),
        in_specs=[vmem_spec] * 3,
        out_specs=(hbm_spec,) * 3,
        scratch_shapes=[dma((3,))],
        compiler_params=pltpu.CompilerParams(vmem_limit_bytes=20 * 1024 * 1024),
        name="store",
    )(*outs)
    return gate_grad.reshape(mp * rows, hid), up_grad.reshape(mp * rows, hid), gain_grad


def plain(cotangent, mlp_out, post_gain, down_weight):
    full = cotangent.shape[1]
    forward = mlp_out.astype(jnp.float32)
    upstream = cotangent.astype(jnp.float32)
    root_mean = jnp.sqrt(jnp.mean(forward * forward, axis=1, keepdims=True) + epsilon)
    normed = forward / root_mean
    gain_part = jnp.sum(upstream * normed, axis=0)
    scaled = upstream * post_gain[None, :]
    project_sum = jnp.sum(scaled * forward, axis=1, keepdims=True)
    out_grad = scaled / root_mean - forward * project_sum / (full * root_mean**3)
    hid_units = down_weight.shape[0]
    gain_grad = lax.psum(gain_part, ("dp", "mp"))
    pieces = lax.all_to_all(out_grad, "dp", split_axis=1, concat_axis=0, tiled=True)
    partial_value = jnp.dot(
        lax.all_gather(pieces, "mp", axis=0, tiled=True),
        down_weight.astype(jnp.float32).T,
        precision=lax.Precision.HIGHEST,
    )
    dp_count = lax.axis_size("dp")
    mp_count = lax.axis_size("mp")
    row_count = out_grad.shape[0]
    partial_value = partial_value.reshape(mp_count, dp_count * row_count, hid_units)
    summed = lax.psum_scatter(partial_value, "dp", scatter_dimension=1, tiled=True)
    return summed.reshape(mp_count * row_count, hid_units), gain_grad


def tile_of(hid):
    return next((t for t in (512, 256, 128) if hid % t == 0), 0)


def local(dp, mp, cotangent, mlp_out, post_gain, down_weight, gate_pre, up_pre):
    rows = cotangent.shape[0]
    hid, feat = down_weight.shape
    span = mp * rows
    held_bytes = span * hid * (2 * 12 + 4 + 12) + 4 * hid * feat + 20 * span * feat
    tiled = rows % 16 == 0 and tile_of(hid) > 0 and feat % LANES == 0
    paired = dp == 4 and mp % 4 == 0
    if tiled and paired and held_bytes < 60 * 1024 * 1024:
        return fused(dp, mp, cotangent, mlp_out, post_gain, down_weight, gate_pre, up_pre)
    hidden_grad, gain_grad = plain(cotangent, mlp_out, post_gain, down_weight)
    gate_val = gate_pre.astype(jnp.float32)
    up_val = up_pre.astype(jnp.float32)
    act_val, pull_back = jax.vjp(gelu_tanh, gate_val)
    gate_grad = pull_back(hidden_grad * up_val)[0]
    up_grad = hidden_grad * act_val
    return (gate_grad, up_grad, gain_grad)


def solution(mesh):
    return jax.shard_map(
        functools.partial(local, mesh.shape["dp"], mesh.shape["mp"]),
        mesh=mesh,
        in_specs=(
            P(("dp", "mp"), None),
            P(("dp", "mp"), None),
            P(),
            P("mp", "dp"),
            P("dp", "mp"),
            P("dp", "mp"),
        ),
        out_specs=(P("dp", "mp"), P("dp", "mp"), P()),
        check_vma=False,
    )
```

```python
import functools
import math

import jax
import jax.numpy as jnp
from jax import lax
from jax.experimental import pallas as pl
from jax.experimental.pallas import tpu as pltpu
from jax.sharding import PartitionSpec as P

MESH = pl.DeviceIdType.MESH
LANES = 128
WEIGHT_MAX = 0.09375
KEPT = 2

epsilon = 1e-06


def gelu_tanh(values):
    return jax.nn.gelu(values, approximate=True)


def encode(v):
    v2 = v * v
    v4 = v2 * v2
    return (v2 * v * v4 * jnp.abs(v)).astype(jnp.bfloat16)


def decode(codes):
    b = codes.astype(jnp.float32)
    size = jnp.abs(b)
    root = jnp.exp2(jnp.log2(size) * 0.125)
    root = jnp.where(size > 0, root, 0.0)
    return jnp.where(b < 0, -root, root)


def groups_of(mp):
    away = [(q, 1) for q in range(4)] + [(q, 2) for q in range(4, mp, 2)]
    home = [(0, 3), (3, mp - 3)]
    order = [(0, g) for g in range(len(away))]
    order.insert(len(away) - 1, (1, 0))
    order.append((1, 1))
    return away, home, order


def kernel(
    dp, mp, gain, tile, wide,
    c_hbm, y_hbm, post_hbm, w_hbm, gate_hbm, up_hbm, gate_out, up_out, gain_out,
    c_ref, y_ref, post_ref, w_ref, wt_ref, gate_ref, up_ref,
    code, grad, size_ref, lhs, mine, dsend, drecv, xsend, got,
    gsend_a, grecv_a, gsum, grecv_b, gblock, gall,
    in_sem, w_sem, act_sem, a_send, a_recv, s_send, s_recv, ga_send, ga_recv, gb_send, gb_recv, go_send, go_recv,
    hello, z_send, y_send, g_recv, d_send, d_recv, x_send, x_recv,
):
    d, m = lax.axis_index("dp"), lax.axis_index("mp")
    nz = mp // 2
    x, core = d // 2, lax.rem(d, 2)
    z, y = m // 2, lax.rem(m, 2)
    rows, full = c_ref.shape
    hid, feat = w_ref.shape
    tiles = hid // tile
    away, home, order = groups_of(mp)

    def remote(src, dst, send, recv, dev):
        return pltpu.make_async_remote_copy(
            src_ref=src, dst_ref=dst, send_sem=send, recv_sem=recv, device_id=dev, device_id_type=MESH
        )

    first = [
        pltpu.make_async_copy(y_hbm, y_ref, in_sem.at[0]),
        pltpu.make_async_copy(c_hbm, c_ref, in_sem.at[1]),
        pltpu.make_async_copy(post_hbm, post_ref, in_sem.at[2]),
    ]
    for copy in first:
        copy.start()

    def many(h, g):
        return 1 if h == 0 and g < 2 else wide

    def slot(h, g):
        n = order.index((h, g))
        return sum(tiles // many(*one) for one in order[:n])

    def lag(h, g):
        return min(3, tiles) if many(h, g) == 1 else min(2, tiles // wide)

    def w_copy(i):
        units = pl.ds(pl.multiple_of(i * tile, tile), tile)
        return pltpu.make_async_copy(w_hbm.at[units, :], w_ref.at[units, :], w_sem.at[i])

    for i in range(tiles):
        w_copy(i).start(priority=1)
    acts = [
        pltpu.make_async_copy(gate_hbm, gate_ref, act_sem.at[0]),
        pltpu.make_async_copy(up_hbm, up_ref, act_sem.at[1]),
    ]
    barrier = pltpu.get_barrier_semaphore()
    for j in range(1, dp):
        pl.semaphore_signal(barrier, inc=1, device_id=(lax.rem(d + j, dp), m), device_id_type=MESH)
    for j in range(1, mp):
        @pl.when(m + j < mp)
        def _():
            pl.semaphore_signal(barrier, inc=1, device_id=(d, m + j), device_id_type=MESH)

    for copy in first:
        copy.wait()
    forward = y_ref[...].astype(jnp.float32)
    upstream = c_ref[...].astype(jnp.float32)
    inv = 1.0 / jnp.sqrt(jnp.mean(forward * forward, axis=1, keepdims=True) + epsilon)
    normed = forward * inv
    scaled = upstream * post_ref[...].reshape(1, full)
    mean_prod = jnp.sum(scaled * normed, axis=1, keepdims=True) * (1.0 / full)
    out_grad = (scaled - normed * mean_prod) * inv
    top = jnp.max(jnp.abs(out_grad), axis=1, keepdims=True)
    top = jnp.where(top > 1e-37, top, 1.0)
    codes = encode(out_grad * (gain / top))
    for t in range(dp):
        code[t] = codes[:, t * feat:(t + 1) * feat]
    grad[1, m, core] = code[d]
    size_ref[m] = jnp.broadcast_to(top * (1.0 / gain), (rows, LANES))

    pl.semaphore_wait(barrier, dp - 1 + m)

    def a_far(c):
        t = 2 * (1 - x) + c
        return remote(code.at[t], grad.at[0, m, core], a_send.at[c], a_recv.at[core], (t, m))

    def a_far_wait(c):
        t = 2 * (1 - x) + c
        return remote(code.at[t], grad.at[0, m, c], a_send.at[c], a_recv.at[c], (t, m))

    def a_near():
        t = 2 * x + 1 - core
        return remote(code.at[t], grad.at[1, m, core], a_send.at[2], a_recv.at[2], (t, m))

    for c in range(2):
        a_far(c).start()
    a_near().start()

    for j in range(1, mp):
        @pl.when(m - j >= 0)
        def _():
            pl.semaphore_signal(hello.at[m], inc=1, device_id=(d, m - j), device_id_type=MESH)

    def greet(mc):
        @pl.when(mc > m)
        def _():
            pl.semaphore_wait(hello.at[mc], 1)

    gain_part = jnp.sum(upstream * normed, axis=0, keepdims=True)
    for t in range(dp):
        gsend_a[t] = gain_part[:, t * feat:(t + 1) * feat]

    def ga_copy(j):
        t = lax.rem(d + j, dp)
        return remote(gsend_a.at[t], grecv_a.at[j], ga_send, ga_recv, (t, m))

    def ga_all():
        return remote(gsend_a.at[pl.ds(1, dp - 1)], grecv_a.at[pl.ds(1, dp - 1)], ga_send, ga_recv, (lax.rem(d + 1, dp), m))

    for j in range(1, dp):
        ga_copy(j).start()

    def turn_over(i, carry):
        units = pl.ds(pl.multiple_of(i * (wide * tile), wide * tile), wide * tile)
        for k in range(wide):
            w_copy(i * wide + k).wait()
        wt_ref[:, units] = w_ref[units, :].T
        return carry

    lax.fori_loop(0, tiles // wide, turn_over, 0)
    for copy in acts:
        copy.start()

    def s_copy(j):
        return remote(size_ref.at[m], size_ref.at[m], s_send, s_recv, (d, lax.rem(m + j, mp)))

    def s_all():
        some = pl.ds(0, mp - 1)
        return remote(size_ref.at[some], size_ref.at[some], s_send, s_recv, (d, lax.rem(m + 1, mp)))

    def place_z(p):
        low = jnp.minimum(z, nz - 1 - z)
        odd = p % 2
        near = z - odd * ((p + 1) // 2) + (1 - odd) * (p // 2)
        up = jnp.where(2 * z < nz - 1, 1, -1)
        return jnp.where(p <= 2 * low, near, z + up * (p - low))

    def level(q):
        if q < 4:
            return 1, q == 2
        return (q - 2, True) if q < nz + 2 else (q - nz, False)

    def place(q):
        if q == 0:
            return m
        if q == 1:
            return 2 * z + 1 - y
        p, same = level(q)
        return 2 * place_z(p) + (y if same else 1 - y)

    def z_copy(h, p):
        return remote(grad.at[h, m], grad.at[h, m], z_send, g_recv.at[h, m], (d, 2 * place_z(p) + y))

    def y_copy(h, p):
        mc = 2 * place_z(p) + y if p else m
        return remote(grad.at[h, mc], grad.at[h, mc], y_send, g_recv.at[h, mc], (d, 2 * z + 1 - y))

    def g_wait(h, q):
        mc = place(q)
        remote(grad.at[h, mc], grad.at[h, mc], y_send, g_recv.at[h, mc], (d, 2 * z + 1 - y)).wait_recv()

    def spread_z(h, low, high):
        for p in range(1, nz):
            away_by = jnp.abs(place_z(p) - z)

            @pl.when(jnp.logical_and(away_by >= low, away_by <= high))
            def _():
                z_copy(h, p).start()

    def d_copy(h, g, i):
        q, n = (away, home)[h][g]
        at, some = pl.ds(q * rows, n * rows), pl.ds(i * many(h, g), many(h, g))
        return remote(
            dsend.at[h, some, at, :], drecv.at[h, some, at, :], d_send, d_recv.at[slot(h, g) + i],
            (2 * x + 1 - core, m),
        )

    def x_copy(g, i):
        q, n = away[g]
        at, some = pl.ds(q * rows, n * rows), pl.ds(i * many(0, g), many(0, g))
        return remote(
            xsend.at[some, at, :], got.at[some, at, :], x_send, x_recv.at[g if g < 3 else 3 + (g - 3) * (tiles // wide) + i], (2 * (1 - x) + core, m)
        )

    def unpack(h, g):
        q0, n = (away, home)[h][g]
        base, span = 4 * q0 * rows, n * rows
        for k in range(n):
            mc = place(q0 + k)
            for s in range(2):
                value = decode(grad[h, mc, core if s == 0 else 1 - core])
                high = value.astype(jnp.bfloat16)
                at = base + s * span + k * rows
                lhs[h, at:at + rows, :] = high
                lhs[h, at + 2 * span:at + 2 * span + rows, :] = (value - high.astype(jnp.float32)).astype(jnp.bfloat16)

    def compute(h, g, i):
        q, n = (away, home)[h][g]
        base, span = 4 * q * rows, n * rows
        width = many(h, g) * tile
        units = pl.ds(pl.multiple_of(i * width, width), width)
        both = lax.dot_general(
            lhs[h, base:base + 4 * span, :], wt_ref[:, units], (((1,), (0,)), ((), ())),
            preferred_element_type=jnp.float32,
        )
        both = both[:2 * span] + both[2 * span:]
        for k in range(many(h, g)):
            cols = slice(k * tile, (k + 1) * tile)
            mine[h, i * many(h, g) + k, q * rows:q * rows + span, :] = both[:span, cols]
            dsend[h, i * many(h, g) + k, q * rows:q * rows + span, :] = both[span:, cols]
        d_copy(h, g, i).start()

    def reduce(h, g, i):
        d_copy(h, g, i).wait_recv()
        if h == 0:
            q, n = away[g]
            at = slice(q * rows, (q + n) * rows)
            for k in range(many(h, g)):
                t = i * many(h, g) + k
                xsend[t, at, :] = encode(mine[0, t, at, :] + drecv[0, t, at, :])
            x_copy(g, i).start()

    def steps(h, g):
        return tiles // many(h, g)

    last = len(away) - 1

    def run(n, start=0, stop=None):
        h, g = order[n]
        late = lag(h, g)
        left = KEPT if n == 1 else lag(*order[n - 1]) if 1 < n < len(order) - 1 else 0
        each = -(-left // steps(h, g))

        def one(i, carry):
            compute(h, g, i)
            for k in range(each):
                j = i * each + k

                @pl.when(j < left)
                def _():
                    reduce(*order[n - 1], steps(*order[n - 1]) - left + j)

            @pl.when(i >= late)
            def _():
                reduce(h, g, i - late)

            return carry

        lax.fori_loop(start, steps(h, g) if stop is None else stop, one, 0)

    def flush(n, keep=0):
        h, g = order[n]

        def one(i, carry):
            reduce(h, g, i)
            return carry

        lax.fori_loop(steps(h, g) - lag(h, g), steps(h, g) - keep, one, 0)

    waited = [{0}, {0}]

    passed = [{0}, {0}]

    def arrive(h, q):
        if q in waited[h]:
            return
        waited[h].add(q)
        g_wait(h, q)

    def relay(h, p):
        if p < nz and p not in passed[h]:
            passed[h].add(p)
            arrive(h, next(q for q in range(2, mp) if level(q) == (p, True)))
            y_copy(h, p).start()

    def ready(h, g):
        q0, n = (away, home)[h][g]
        for q in range(q0, q0 + n):
            if h == 0 and q > 2 and level(q)[1]:
                relay(h, level(q)[0])
            arrive(h, q)
        unpack(h, g)

    for c in range(2):
        a_far_wait(c).wait_recv()
    greet(place(1))
    y_copy(0, 0).start()
    for p in range(1, nz):
        greet(2 * place_z(p) + y)
    spread_z(0, 1, 1)

    def near_wait():
        remote(code.at[0], grad.at[1, m, 1 - core], a_send.at[2], a_recv.at[2], (2 * x + 1 - core, m)).wait_recv()

    def gb_copy(j):
        return remote(gsum, grecv_b.at[j], gb_send, gb_recv, (d, lax.rem(m + j, mp)))

    def gb_all():
        some = grecv_b.at[pl.ds(1, mp - 1)]
        return remote(some, some, gb_send, gb_recv, (d, lax.rem(m + 1, mp)))

    def go_copy(j):
        return remote(gblock, gall.at[d], go_send, go_recv, (lax.rem(d + j, dp), m))

    def go_all():
        some = gall.at[pl.ds(0, dp - 1)]
        return remote(some, some, go_send, go_recv, (lax.rem(d + 1, dp), m))

    slope = math.sqrt(2.0 / math.pi)

    def finish(g, i):
        q0, n = away[g]
        if g >= 3:
            x_copy(g, i).wait_recv()
        for k in range(many(0, g)):
            t = i * many(0, g) + k
            cols = pl.ds(pl.multiple_of(t * tile, tile), tile)
            for q in range(q0, q0 + n):
                mc = place(q)
                at = slice(q * rows, (q + 1) * rows)
                value = mine[1, t, at, :] + drecv[1, t, at, :] + decode(got[t, at, :])
                value = value * size_ref[mc][:, :1]
                gate = gate_ref[mc, :, cols].astype(jnp.float32)
                up = up_ref[mc, :, cols].astype(jnp.float32)
                square = gate * gate
                bent = jnp.tanh(gate * (slope + (slope * 0.044715) * square))
                half = 0.5 + 0.5 * bent
                up_out[mc, :, cols] = value * (gate * half)
                turn = half + (0.5 * gate) * (1.0 - bent * bent) * (slope + (3.0 * slope * 0.044715) * square)
                gate_out[mc, :, cols] = (value * up) * turn

    def finish_all(g):
        at = pl.ds(away[g][0] * rows, away[g][1] * rows)
        whole = got.at[:, at, :]
        remote(whole, whole, x_send, x_recv.at[g], (2 * (1 - x) + core, m)).wait_recv()

        def one(i, carry):
            finish(g, i)
            return carry

        lax.fori_loop(0, steps(0, g), one, 0)

    for n in range(len(order)):
        h, g = order[n]
        ready(h, g)
        if n == 0:
            run(n, 0, (tiles + 1) // 2)
            spread_z(0, 2, 2)
            run(n, (tiles + 1) // 2)
            flush(n, KEPT)
            near_wait()
            for p in range(1, nz):
                greet(2 * place_z(p) + 1 - y)
            for j in range(1, mp):
                s_copy(j).start()
            ga_all().wait_recv()
            total = gsend_a[d]
            for j in range(1, dp):
                total = total + grecv_a[j]
            gsum[...] = total
            for j in range(1, mp):
                gb_copy(j).start()
        elif n == 1:
            spread_z(0, 3, nz)
            relay(0, 1)
            run(n, 0, (tiles + 1) // 2)
            y_copy(1, 0).start()
            run(n, (tiles + 1) // 2)
        elif n == 2:
            run(n)
            spread_z(1, 1, 1)
        elif n == 3:
            run(n, 0, steps(h, g) - 1)
            spread_z(1, 2, 2)
            relay(0, 2)
            run(n, steps(h, g) - 1)
        elif n == 4:
            run(n, 0, 1)
            spread_z(1, 3, nz)
            run(n, 1)
        elif (h, g) == (1, 0):
            run(n, 0, steps(h, g) - 1)
            relay(1, 1)
            run(n, steps(h, g) - 1)
        elif (h, g) == (0, last):
            run(n, 0, 1)
            relay(1, 2)
            run(n, 1)
            for p in range(3, nz):
                relay(1, p)
        else:
            run(n)
        if (h, g) == (0, last):
            gtotal = gsum[...]
            gb_all().wait()
            for j in range(1, mp):
                gtotal = gtotal + grecv_b[j]
            gblock[...] = gtotal
            gall[d] = gtotal
            for j in range(1, dp):
                go_copy(j).start()
            s_all().wait_recv()
            for copy in acts:
                copy.wait()
            flush(n)
            for g in range(3):
                finish_all(g)

    late = steps(1, 1) - lag(1, 1)

    def end(i, carry):
        @pl.when(i >= late)
        def _():
            reduce(1, 1, i)

        for g in range(3, last):
            finish(g, i)
        return carry

    def end_last(i, carry):
        finish(last, i)
        return carry

    lax.fori_loop(0, steps(1, 1), end, 0)
    lax.fori_loop(0, steps(1, 1), end_last, 0)

    go_all().wait()
    for t in range(dp):
        gain_out[t * feat:(t + 1) * feat] = gall[t].reshape(feat)

    a_far(0).wait_send()
    a_far(1).wait_send()
    a_near().wait_send()
    ga_all().wait_send()
    s_all().wait_send()
    remote(grad.at[0], grad.at[0], y_send, g_recv.at[0, m], (d, 2 * z + 1 - y)).wait_send()
    some = grad.at[0, pl.ds(0, 2 * (nz - 1))]
    remote(some, some, z_send, g_recv.at[0, m], (d, 2 * z + 1 - y)).wait_send()
    remote(dsend, drecv, d_send, d_recv.at[0], (2 * x + 1 - core, m)).wait_send()
    remote(xsend, got, x_send, x_recv.at[0], (2 * (1 - x) + core, m)).wait_send()


def store(gate_in, up_in, gain_in, gate_to, up_to, gain_to, sem):
    copies = [
        pltpu.make_async_copy(src, dst, sem.at[n])
        for n, (src, dst) in enumerate(((gate_in, gate_to), (up_in, up_to), (gain_in, gain_to)))
    ]
    for copy in copies:
        copy.start()
    for copy in copies:
        copy.wait()


def fused(dp, mp, cotangent, mlp_out, post_gain, down_weight, gate_pre, up_pre):
    rows, full = cotangent.shape
    hid, feat = down_weight.shape
    nz = mp // 2
    gain = 2.0 ** math.floor(15.8 - math.log2(full * WEIGHT_MAX))
    tile = tile_of(hid)
    tiles = hid // tile
    wide = next(k for k in (3, 2, 1) if tiles % k == 0)
    bf, f32 = jnp.bfloat16, jnp.float32
    dma = pltpu.SemaphoreType.DMA
    span = mp * rows
    steps = 2 * tiles + tiles // wide * (len(groups_of(mp)[2]) - 2)
    hbm_spec = pl.BlockSpec(memory_space=pltpu.HBM)
    vmem_spec = pl.BlockSpec(memory_space=pltpu.VMEM)
    gate_grad, up_grad, gain_grad = pl.pallas_call(
        functools.partial(kernel, dp, mp, gain, tile, wide),
        out_shape=(
            pltpu.VMEM((mp, rows, hid), f32),
            pltpu.VMEM((mp, rows, hid), f32),
            pltpu.VMEM((full,), f32),
        ),
        in_specs=[hbm_spec] * 6,
        out_specs=(vmem_spec,) * 3,
        scratch_shapes=[
            pltpu.VMEM((rows, full), bf),
            pltpu.VMEM((rows, full), bf),
            pltpu.VMEM((full,), f32),
            pltpu.VMEM((hid, feat), bf),
            pltpu.VMEM((feat, hid), bf),
            pltpu.VMEM((mp, rows, hid), bf),
            pltpu.VMEM((mp, rows, hid), bf),
            pltpu.VMEM((dp, rows, feat), bf),
            pltpu.VMEM((2, mp, 2, rows, feat), bf),
            pltpu.VMEM((mp, rows, LANES), f32),
            pltpu.VMEM((2, 4 * span, feat), bf),
            pltpu.VMEM((2, tiles, span, tile), f32),
            pltpu.VMEM((2, tiles, span, tile), f32),
            pltpu.VMEM((2, tiles, span, tile), f32),
            pltpu.VMEM((tiles, span, tile), bf),
            pltpu.VMEM((tiles, span, tile), bf),
            pltpu.VMEM((dp, 1, feat), f32),
            pltpu.VMEM((dp, 1, feat), f32),
            pltpu.VMEM((1, feat), f32),
            pltpu.VMEM((mp, 1, feat), f32),
            pltpu.VMEM((1, feat), f32),
            pltpu.VMEM((dp, 1, feat), f32),
            dma((3,)), dma((tiles,)), dma((2,)), dma((3,)), dma((3,)), dma, dma,
            dma, dma, dma, dma, dma, dma,
            pltpu.SemaphoreType.REGULAR((mp,)), dma, dma, dma((2, mp)),
            dma, dma((steps,)), dma, dma((3 + tiles // wide * (len(groups_of(mp)[0]) - 3),)),
        ],
        compiler_params=pltpu.CompilerParams(
            collective_id=0, has_side_effects=True, vmem_limit_bytes=52 * 1024 * 1024
        ),
        name="norm_gather_project_reduce",
    )(*(
        pltpu.with_memory_space_constraint(value, pltpu.HBM)
        for value in (
            cotangent, mlp_out, post_gain, down_weight,
            gate_pre.reshape(mp, rows, hid), up_pre.reshape(mp, rows, hid),
        )
    ))
    outs = (gate_grad, up_grad, gain_grad)
    gate_grad, up_grad, gain_grad = pl.pallas_call(
        store,
        out_shape=tuple(pltpu.HBM(value.shape, f32) for value in outs),
        in_specs=[vmem_spec] * 3,
        out_specs=(hbm_spec,) * 3,
        scratch_shapes=[dma((3,))],
        compiler_params=pltpu.CompilerParams(vmem_limit_bytes=20 * 1024 * 1024),
        name="store",
    )(*outs)
    return gate_grad.reshape(mp * rows, hid), up_grad.reshape(mp * rows, hid), gain_grad


def plain(cotangent, mlp_out, post_gain, down_weight):
    full = cotangent.shape[1]
    forward = mlp_out.astype(jnp.float32)
    upstream = cotangent.astype(jnp.float32)
    root_mean = jnp.sqrt(jnp.mean(forward * forward, axis=1, keepdims=True) + epsilon)
    normed = forward / root_mean
    gain_part = jnp.sum(upstream * normed, axis=0)
    scaled = upstream * post_gain[None, :]
    project_sum = jnp.sum(scaled * forward, axis=1, keepdims=True)
    out_grad = scaled / root_mean - forward * project_sum / (full * root_mean**3)
    hid_units = down_weight.shape[0]
    gain_grad = lax.psum(gain_part, ("dp", "mp"))
    pieces = lax.all_to_all(out_grad, "dp", split_axis=1, concat_axis=0, tiled=True)
    partial_value = jnp.dot(
        lax.all_gather(pieces, "mp", axis=0, tiled=True),
        down_weight.astype(jnp.float32).T,
        precision=lax.Precision.HIGHEST,
    )
    dp_count = lax.axis_size("dp")
    mp_count = lax.axis_size("mp")
    row_count = out_grad.shape[0]
    partial_value = partial_value.reshape(mp_count, dp_count * row_count, hid_units)
    summed = lax.psum_scatter(partial_value, "dp", scatter_dimension=1, tiled=True)
    return summed.reshape(mp_count * row_count, hid_units), gain_grad


def tile_of(hid):
    return next((t for t in (512, 256, 128) if hid % t == 0), 0)


def local(dp, mp, cotangent, mlp_out, post_gain, down_weight, gate_pre, up_pre):
    rows = cotangent.shape[0]
    hid, feat = down_weight.shape
    span = mp * rows
    held_bytes = span * hid * (2 * 12 + 4 + 12) + 4 * hid * feat + 20 * span * feat
    tiled = rows % 16 == 0 and tile_of(hid) > 0 and feat % LANES == 0
    paired = dp == 4 and mp % 4 == 0
    if tiled and paired and held_bytes < 60 * 1024 * 1024:
        return fused(dp, mp, cotangent, mlp_out, post_gain, down_weight, gate_pre, up_pre)
    hidden_grad, gain_grad = plain(cotangent, mlp_out, post_gain, down_weight)
    gate_val = gate_pre.astype(jnp.float32)
    up_val = up_pre.astype(jnp.float32)
    act_val, pull_back = jax.vjp(gelu_tanh, gate_val)
    gate_grad = pull_back(hidden_grad * up_val)[0]
    up_grad = hidden_grad * act_val
    return (gate_grad, up_grad, gain_grad)


def solution(mesh):
    return jax.shard_map(
        functools.partial(local, mesh.shape["dp"], mesh.shape["mp"]),
        mesh=mesh,
        in_specs=(
            P(("dp", "mp"), None),
            P(("dp", "mp"), None),
            P(),
            P("mp", "dp"),
            P("dp", "mp"),
            P("dp", "mp"),
        ),
        out_specs=(P("dp", "mp"), P("dp", "mp"), P()),
        check_vma=False,
    )
```

```python
import functools
import math

import jax
import jax.numpy as jnp
from jax import lax
from jax.experimental import pallas as pl
from jax.experimental.pallas import tpu as pltpu
from jax.sharding import PartitionSpec as P

MESH = pl.DeviceIdType.MESH
LANES = 128
WEIGHT_MAX = 0.09375
KEPT = 2

epsilon = 1e-06


def gelu_tanh(values):
    return jax.nn.gelu(values, approximate=True)


def encode(v):
    v2 = v * v
    v4 = v2 * v2
    return (v2 * v * v4 * jnp.abs(v)).astype(jnp.bfloat16)


def decode(codes):
    b = codes.astype(jnp.float32)
    size = jnp.abs(b)
    root = jnp.exp2(jnp.log2(size) * 0.125)
    root = jnp.where(size > 0, root, 0.0)
    return jnp.where(b < 0, -root, root)


def groups_of(mp):
    away = [(q, 1) for q in range(4)] + [(q, 2) for q in range(4, mp, 2)]
    home = [(0, 3), (3, mp - 5), (mp - 2, 2)]
    order = [(0, g) for g in range(len(away))]
    order.insert(len(away) - 1, (1, 0))
    order += [(1, 1), (1, 2)]
    return away, home, order


def kernel(
    dp, mp, gain, tile, wide,
    c_hbm, y_hbm, post_hbm, w_hbm, gate_hbm, up_hbm, gate_out, up_out, gain_out,
    c_ref, y_ref, post_ref, w_ref, wt_ref, gate_ref, up_ref,
    code, grad, size_ref, lhs, mine, dsend, drecv, xsend, got,
    gsend_a, grecv_a, gsum, grecv_b, gblock, gall,
    in_sem, w_sem, act_sem, a_send, a_recv, s_send, s_recv, ga_send, ga_recv, gb_send, gb_recv, go_send, go_recv,
    hello, z_send, y_send, g_recv, d_send, d_recv, x_send, x_recv,
):
    d, m = lax.axis_index("dp"), lax.axis_index("mp")
    nz = mp // 2
    x, core = d // 2, lax.rem(d, 2)
    z, y = m // 2, lax.rem(m, 2)
    rows, full = c_ref.shape
    hid, feat = w_ref.shape
    tiles = hid // tile
    away, home, order = groups_of(mp)

    def remote(src, dst, send, recv, dev):
        return pltpu.make_async_remote_copy(
            src_ref=src, dst_ref=dst, send_sem=send, recv_sem=recv, device_id=dev, device_id_type=MESH
        )

    first = [
        pltpu.make_async_copy(y_hbm, y_ref, in_sem.at[0]),
        pltpu.make_async_copy(c_hbm, c_ref, in_sem.at[1]),
        pltpu.make_async_copy(post_hbm, post_ref, in_sem.at[2]),
    ]
    for copy in first:
        copy.start()

    def many(h, g):
        return 1 if h == 0 and g < 2 else wide

    def slot(h, g):
        n = order.index((h, g))
        return sum(tiles // many(*one) for one in order[:n])

    def lag(h, g):
        return min(3, tiles) if many(h, g) == 1 else min(2, tiles // wide)

    def w_copy(i):
        units = pl.ds(pl.multiple_of(i * tile, tile), tile)
        return pltpu.make_async_copy(w_hbm.at[units, :], w_ref.at[units, :], w_sem.at[i])

    for i in range(tiles):
        w_copy(i).start(priority=1)
    acts = [
        pltpu.make_async_copy(gate_hbm, gate_ref, act_sem.at[0]),
        pltpu.make_async_copy(up_hbm, up_ref, act_sem.at[1]),
    ]
    barrier = pltpu.get_barrier_semaphore()
    for j in range(1, dp):
        pl.semaphore_signal(barrier, inc=1, device_id=(lax.rem(d + j, dp), m), device_id_type=MESH)
    for j in range(1, mp):
        @pl.when(m + j < mp)
        def _():
            pl.semaphore_signal(barrier, inc=1, device_id=(d, m + j), device_id_type=MESH)

    for copy in first:
        copy.wait()
    forward = y_ref[...].astype(jnp.float32)
    upstream = c_ref[...].astype(jnp.float32)
    inv = 1.0 / jnp.sqrt(jnp.mean(forward * forward, axis=1, keepdims=True) + epsilon)
    normed = forward * inv
    scaled = upstream * post_ref[...].reshape(1, full)
    mean_prod = jnp.sum(scaled * normed, axis=1, keepdims=True) * (1.0 / full)
    out_grad = (scaled - normed * mean_prod) * inv
    top = jnp.max(jnp.abs(out_grad), axis=1, keepdims=True)
    top = jnp.where(top > 1e-37, top, 1.0)
    codes = encode(out_grad * (gain / top))
    for t in range(dp):
        code[t] = codes[:, t * feat:(t + 1) * feat]
    grad[1, m, core] = code[d]
    size_ref[m] = jnp.broadcast_to(top * (1.0 / gain), (rows, LANES))

    pl.semaphore_wait(barrier, dp - 1 + m)

    def a_far(c):
        t = 2 * (1 - x) + c
        return remote(code.at[t], grad.at[0, m, core], a_send.at[c], a_recv.at[core], (t, m))

    def a_far_wait(c):
        t = 2 * (1 - x) + c
        return remote(code.at[t], grad.at[0, m, c], a_send.at[c], a_recv.at[c], (t, m))

    def a_near():
        t = 2 * x + 1 - core
        return remote(code.at[t], grad.at[1, m, core], a_send.at[2], a_recv.at[2], (t, m))

    for c in range(2):
        a_far(c).start()
    a_near().start()

    for j in range(1, mp):
        @pl.when(m - j >= 0)
        def _():
            pl.semaphore_signal(hello.at[m], inc=1, device_id=(d, m - j), device_id_type=MESH)

    def greet(mc):
        @pl.when(mc > m)
        def _():
            pl.semaphore_wait(hello.at[mc], 1)

    gain_part = jnp.sum(upstream * normed, axis=0, keepdims=True)
    for t in range(dp):
        gsend_a[t] = gain_part[:, t * feat:(t + 1) * feat]

    def ga_copy(j):
        t = lax.rem(d + j, dp)
        return remote(gsend_a.at[t], grecv_a.at[j], ga_send, ga_recv, (t, m))

    def ga_all():
        return remote(gsend_a.at[pl.ds(1, dp - 1)], grecv_a.at[pl.ds(1, dp - 1)], ga_send, ga_recv, (lax.rem(d + 1, dp), m))

    for j in range(1, dp):
        ga_copy(j).start()

    def turn_over(i, carry):
        units = pl.ds(pl.multiple_of(i * (wide * tile), wide * tile), wide * tile)
        for k in range(wide):
            w_copy(i * wide + k).wait()
        wt_ref[:, units] = w_ref[units, :].T
        return carry

    lax.fori_loop(0, tiles // wide, turn_over, 0)
    for copy in acts:
        copy.start()

    def s_copy(j):
        return remote(size_ref.at[m], size_ref.at[m], s_send, s_recv, (d, lax.rem(m + j, mp)))

    def s_all():
        some = pl.ds(0, mp - 1)
        return remote(size_ref.at[some], size_ref.at[some], s_send, s_recv, (d, lax.rem(m + 1, mp)))

    def place_z(p):
        low = jnp.minimum(z, nz - 1 - z)
        odd = p % 2
        near = z - odd * ((p + 1) // 2) + (1 - odd) * (p // 2)
        up = jnp.where(2 * z < nz - 1, 1, -1)
        return jnp.where(p <= 2 * low, near, z + up * (p - low))

    def level(q):
        if q < 4:
            return 1, q == 2
        return (q - 2, True) if q < nz + 2 else (q - nz, False)

    def place(q):
        if q == 0:
            return m
        if q == 1:
            return 2 * z + 1 - y
        p, same = level(q)
        return 2 * place_z(p) + (y if same else 1 - y)

    def z_copy(h, p):
        return remote(grad.at[h, m], grad.at[h, m], z_send, g_recv.at[h, m], (d, 2 * place_z(p) + y))

    def y_copy(h, p):
        mc = 2 * place_z(p) + y if p else m
        return remote(grad.at[h, mc], grad.at[h, mc], y_send, g_recv.at[h, mc], (d, 2 * z + 1 - y))

    def g_wait(h, q):
        mc = place(q)
        remote(grad.at[h, mc], grad.at[h, mc], y_send, g_recv.at[h, mc], (d, 2 * z + 1 - y)).wait_recv()

    def spread_z(h, low, high):
        for p in range(1, nz):
            away_by = jnp.abs(place_z(p) - z)

            @pl.when(jnp.logical_and(away_by >= low, away_by <= high))
            def _():
                z_copy(h, p).start()

    def d_copy(h, g, i):
        q, n = (away, home)[h][g]
        at, some = pl.ds(q * rows, n * rows), pl.ds(i * many(h, g), many(h, g))
        return remote(
            dsend.at[h, some, at, :], drecv.at[h, some, at, :], d_send, d_recv.at[slot(h, g) + i],
            (2 * x + 1 - core, m),
        )

    def x_copy(g, i):
        q, n = away[g]
        at, some = pl.ds(q * rows, n * rows), pl.ds(i * many(0, g), many(0, g))
        return remote(
            xsend.at[some, at, :], got.at[some, at, :], x_send, x_recv.at[g if g < 3 else 3 + (g - 3) * (tiles // wide) + i], (2 * (1 - x) + core, m)
        )

    def unpack(h, g, these):
        q0, n = (away, home)[h][g]
        base, span = 4 * q0 * rows, n * rows
        for k in these:
            mc = place(q0 + k)
            for s in range(2):
                value = decode(grad[h, mc, core if s == 0 else 1 - core])
                high = value.astype(jnp.bfloat16)
                at = base + s * span + k * rows
                lhs[h, at:at + rows, :] = high
                lhs[h, at + 2 * span:at + 2 * span + rows, :] = (value - high.astype(jnp.float32)).astype(jnp.bfloat16)

    def compute(h, g, i):
        q, n = (away, home)[h][g]
        base, span = 4 * q * rows, n * rows
        width = many(h, g) * tile
        units = pl.ds(pl.multiple_of(i * width, width), width)
        both = lax.dot_general(
            lhs[h, base:base + 4 * span, :], wt_ref[:, units], (((1,), (0,)), ((), ())),
            preferred_element_type=jnp.float32,
        )
        both = both[:2 * span] + both[2 * span:]
        for k in range(many(h, g)):
            cols = slice(k * tile, (k + 1) * tile)
            mine[h, i * many(h, g) + k, q * rows:q * rows + span, :] = both[:span, cols]
            dsend[h, i * many(h, g) + k, q * rows:q * rows + span, :] = both[span:, cols]
        d_copy(h, g, i).start()

    def reduce(h, g, i):
        d_copy(h, g, i).wait_recv()
        if h == 0:
            q, n = away[g]
            at = slice(q * rows, (q + n) * rows)
            for k in range(many(h, g)):
                t = i * many(h, g) + k
                xsend[t, at, :] = encode(mine[0, t, at, :] + drecv[0, t, at, :])
            x_copy(g, i).start()

    def steps(h, g):
        return tiles // many(h, g)

    last = len(away) - 1

    def run(n, start=0, stop=None):
        h, g = order[n]
        late = lag(h, g)
        left = KEPT if n == 1 else lag(*order[n - 1]) if 1 < n < len(away) + 1 else 0
        each = -(-left // steps(h, g)) if n < 2 else min(2, left)

        def one(i, carry):
            compute(h, g, i)
            for k in range(each):
                j = i * each + k

                @pl.when(j < left)
                def _():
                    reduce(*order[n - 1], steps(*order[n - 1]) - left + j)

            @pl.when(i >= late)
            def _():
                reduce(h, g, i - late)

            return carry

        lax.fori_loop(start, steps(h, g) if stop is None else stop, one, 0)

    def flush(n, keep=0):
        h, g = order[n]

        def one(i, carry):
            reduce(h, g, i)
            return carry

        lax.fori_loop(steps(h, g) - lag(h, g), steps(h, g) - keep, one, 0)

    waited = [{0}, {0}]

    passed = [{0}, {0}]

    def arrive(h, q):
        if q in waited[h]:
            return
        waited[h].add(q)
        g_wait(h, q)

    def relay(h, p):
        if p < nz and p not in passed[h]:
            passed[h].add(p)
            arrive(h, next(q for q in range(2, mp) if level(q) == (p, True)))
            y_copy(h, p).start()

    def ready(h, g):
        q0, n = (away, home)[h][g]
        for q in range(q0, q0 + n):
            if h == 0 and q > 2 and level(q)[1]:
                relay(h, level(q)[0])
            arrive(h, q)
            if h == 1:
                unpack(h, g, [q - q0])
        if h == 0:
            unpack(h, g, range(n))

    for c in range(2):
        a_far_wait(c).wait_recv()
    greet(place(1))
    y_copy(0, 0).start()
    for p in range(1, nz):
        greet(2 * place_z(p) + y)
    spread_z(0, 1, 1)

    def near_wait():
        remote(code.at[0], grad.at[1, m, 1 - core], a_send.at[2], a_recv.at[2], (2 * x + 1 - core, m)).wait_recv()

    def gb_copy(j):
        return remote(gsum, grecv_b.at[j], gb_send, gb_recv, (d, lax.rem(m + j, mp)))

    def gb_all():
        some = grecv_b.at[pl.ds(1, mp - 1)]
        return remote(some, some, gb_send, gb_recv, (d, lax.rem(m + 1, mp)))

    def go_copy(j):
        return remote(gblock, gall.at[d], go_send, go_recv, (lax.rem(d + j, dp), m))

    def go_all():
        some = gall.at[pl.ds(0, dp - 1)]
        return remote(some, some, go_send, go_recv, (lax.rem(d + 1, dp), m))

    slope = math.sqrt(2.0 / math.pi)

    def finish(g, i):
        q0, n = away[g]
        if g >= 3:
            x_copy(g, i).wait_recv()
        for k in range(many(0, g)):
            t = i * many(0, g) + k
            cols = pl.ds(pl.multiple_of(t * tile, tile), tile)
            for q in range(q0, q0 + n):
                mc = place(q)
                at = slice(q * rows, (q + 1) * rows)
                value = mine[1, t, at, :] + drecv[1, t, at, :] + decode(got[t, at, :])
                value = value * size_ref[mc][:, :1]
                gate = gate_ref[mc, :, cols].astype(jnp.float32)
                up = up_ref[mc, :, cols].astype(jnp.float32)
                square = gate * gate
                bent = jnp.tanh(gate * (slope + (slope * 0.044715) * square))
                half = 0.5 + 0.5 * bent
                up_out[mc, :, cols] = value * (gate * half)
                turn = half + (0.5 * gate) * (1.0 - bent * bent) * (slope + (3.0 * slope * 0.044715) * square)
                gate_out[mc, :, cols] = (value * up) * turn

    def finish_all(g):
        at = pl.ds(away[g][0] * rows, away[g][1] * rows)
        whole = got.at[:, at, :]
        remote(whole, whole, x_send, x_recv.at[g], (2 * (1 - x) + core, m)).wait_recv()

        def one(i, carry):
            finish(g, i)
            return carry

        lax.fori_loop(0, steps(0, g), one, 0)

    late = steps(1, 1) - lag(1, 1)

    def end(i, carry):
        @pl.when(i >= late)
        def _():
            reduce(1, 1, i)

        for g in range(3, last):
            finish(g, i)
        return carry

    for n in range(len(order)):
        h, g = order[n]
        ready(h, g)
        if n == 0:
            run(n, 0, (tiles + 1) // 2)
            spread_z(0, 2, 2)
            run(n, (tiles + 1) // 2)
            flush(n, KEPT)
            near_wait()
            for p in range(1, nz):
                greet(2 * place_z(p) + 1 - y)
            for j in range(1, mp):
                s_copy(j).start()
            ga_all().wait_recv()
            total = gsend_a[d]
            for j in range(1, dp):
                total = total + grecv_a[j]
            gsum[...] = total
            for j in range(1, mp):
                gb_copy(j).start()
        elif n == 1:
            spread_z(0, 3, nz)
            relay(0, 1)
            run(n, 0, (tiles + 1) // 2)
            y_copy(1, 0).start()
            run(n, (tiles + 1) // 2)
        elif n == 2:
            run(n)
            spread_z(1, 1, 1)
        elif n == 3:
            run(n, 0, steps(h, g) - 1)
            spread_z(1, 2, 2)
            relay(0, 2)
            run(n, steps(h, g) - 1)
        elif n == 4:
            run(n, 0, 1)
            spread_z(1, 3, nz)
            run(n, 1)
        elif (h, g) == (1, 0):
            run(n, 0, steps(h, g) - 1)
            relay(1, 1)
            run(n, steps(h, g) - 1)
        elif (h, g) == (0, last):
            run(n, 0, 1)
            relay(1, 2)
            run(n, 1, 2)
            for p in range(3, nz):
                relay(1, p)
            run(n, 2)
        elif (h, g) == (1, 1):
            run(n)
            lax.fori_loop(0, steps(1, 1), end, 0)
        else:
            run(n)
        if (h, g) == (0, last):
            gtotal = gsum[...]
            gb_all().wait()
            for j in range(1, mp):
                gtotal = gtotal + grecv_b[j]
            gblock[...] = gtotal
            gall[d] = gtotal
            for j in range(1, dp):
                go_copy(j).start()
            s_all().wait_recv()
            for copy in acts:
                copy.wait()
            flush(n, 1)
            finish_all(0)
            reduce(h, g, steps(h, g) - 1)
            for k in range(1, 3):
                finish_all(k)

    def end_last(i, carry):
        @pl.when(i >= late)
        def _():
            reduce(1, 2, i)

        finish(last, i)
        return carry

    go_all().wait()
    for t in range(dp):
        gain_out[t * feat:(t + 1) * feat] = gall[t].reshape(feat)
    lax.fori_loop(0, steps(1, 2), end_last, 0)

    a_far(0).wait_send()
    a_far(1).wait_send()
    a_near().wait_send()
    ga_all().wait_send()
    s_all().wait_send()
    remote(grad.at[0], grad.at[0], y_send, g_recv.at[0, m], (d, 2 * z + 1 - y)).wait_send()
    some = grad.at[0, pl.ds(0, 2 * (nz - 1))]
    remote(some, some, z_send, g_recv.at[0, m], (d, 2 * z + 1 - y)).wait_send()
    remote(dsend, drecv, d_send, d_recv.at[0], (2 * x + 1 - core, m)).wait_send()
    remote(xsend, got, x_send, x_recv.at[0], (2 * (1 - x) + core, m)).wait_send()


def store(gate_in, up_in, gain_in, gate_to, up_to, gain_to, sem):
    pairs = [(gain_in, gain_to)]
    half = gate_in.shape[0] // 2
    for k in range(2):
        some = pl.ds(k * half, half)
        pairs += [(gate_in.at[some], gate_to.at[some]), (up_in.at[some], up_to.at[some])]
    copies = [pltpu.make_async_copy(src, dst, sem.at[n]) for n, (src, dst) in enumerate(pairs)]
    for copy in copies:
        copy.start()
    for copy in copies:
        copy.wait()


def fused(dp, mp, cotangent, mlp_out, post_gain, down_weight, gate_pre, up_pre):
    rows, full = cotangent.shape
    hid, feat = down_weight.shape
    nz = mp // 2
    gain = 2.0 ** math.floor(15.8 - math.log2(full * WEIGHT_MAX))
    tile = tile_of(hid)
    tiles = hid // tile
    wide = next(k for k in (3, 2, 1) if tiles % k == 0)
    bf, f32 = jnp.bfloat16, jnp.float32
    dma = pltpu.SemaphoreType.DMA
    span = mp * rows
    steps = 2 * tiles + tiles // wide * (len(groups_of(mp)[2]) - 2)
    hbm_spec = pl.BlockSpec(memory_space=pltpu.HBM)
    vmem_spec = pl.BlockSpec(memory_space=pltpu.VMEM)
    gate_grad, up_grad, gain_grad = pl.pallas_call(
        functools.partial(kernel, dp, mp, gain, tile, wide),
        out_shape=(
            pltpu.VMEM((mp, rows, hid), f32),
            pltpu.VMEM((mp, rows, hid), f32),
            pltpu.VMEM((full,), f32),
        ),
        in_specs=[hbm_spec] * 6,
        out_specs=(vmem_spec,) * 3,
        scratch_shapes=[
            pltpu.VMEM((rows, full), bf),
            pltpu.VMEM((rows, full), bf),
            pltpu.VMEM((full,), f32),
            pltpu.VMEM((hid, feat), bf),
            pltpu.VMEM((feat, hid), bf),
            pltpu.VMEM((mp, rows, hid), bf),
            pltpu.VMEM((mp, rows, hid), bf),
            pltpu.VMEM((dp, rows, feat), bf),
            pltpu.VMEM((2, mp, 2, rows, feat), bf),
            pltpu.VMEM((mp, rows, LANES), f32),
            pltpu.VMEM((2, 4 * span, feat), bf),
            pltpu.VMEM((2, tiles, span, tile), f32),
            pltpu.VMEM((2, tiles, span, tile), f32),
            pltpu.VMEM((2, tiles, span, tile), f32),
            pltpu.VMEM((tiles, span, tile), bf),
            pltpu.VMEM((tiles, span, tile), bf),
            pltpu.VMEM((dp, 1, feat), f32),
            pltpu.VMEM((dp, 1, feat), f32),
            pltpu.VMEM((1, feat), f32),
            pltpu.VMEM((mp, 1, feat), f32),
            pltpu.VMEM((1, feat), f32),
            pltpu.VMEM((dp, 1, feat), f32),
            dma((3,)), dma((tiles,)), dma((2,)), dma((3,)), dma((3,)), dma, dma,
            dma, dma, dma, dma, dma, dma,
            pltpu.SemaphoreType.REGULAR((mp,)), dma, dma, dma((2, mp)),
            dma, dma((steps,)), dma, dma((3 + tiles // wide * (len(groups_of(mp)[0]) - 3),)),
        ],
        compiler_params=pltpu.CompilerParams(
            collective_id=0, has_side_effects=True, vmem_limit_bytes=52 * 1024 * 1024
        ),
        name="norm_gather_project_reduce",
    )(*(
        pltpu.with_memory_space_constraint(value, pltpu.HBM)
        for value in (
            cotangent, mlp_out, post_gain, down_weight,
            gate_pre.reshape(mp, rows, hid), up_pre.reshape(mp, rows, hid),
        )
    ))
    outs = (gate_grad, up_grad, gain_grad)
    gate_grad, up_grad, gain_grad = pl.pallas_call(
        store,
        out_shape=tuple(pltpu.HBM(value.shape, f32) for value in outs),
        in_specs=[vmem_spec] * 3,
        out_specs=(hbm_spec,) * 3,
        scratch_shapes=[dma((5,))],
        compiler_params=pltpu.CompilerParams(vmem_limit_bytes=20 * 1024 * 1024),
        name="store",
    )(*outs)
    return gate_grad.reshape(mp * rows, hid), up_grad.reshape(mp * rows, hid), gain_grad


def plain(cotangent, mlp_out, post_gain, down_weight):
    full = cotangent.shape[1]
    forward = mlp_out.astype(jnp.float32)
    upstream = cotangent.astype(jnp.float32)
    root_mean = jnp.sqrt(jnp.mean(forward * forward, axis=1, keepdims=True) + epsilon)
    normed = forward / root_mean
    gain_part = jnp.sum(upstream * normed, axis=0)
    scaled = upstream * post_gain[None, :]
    project_sum = jnp.sum(scaled * forward, axis=1, keepdims=True)
    out_grad = scaled / root_mean - forward * project_sum / (full * root_mean**3)
    hid_units = down_weight.shape[0]
    gain_grad = lax.psum(gain_part, ("dp", "mp"))
    pieces = lax.all_to_all(out_grad, "dp", split_axis=1, concat_axis=0, tiled=True)
    partial_value = jnp.dot(
        lax.all_gather(pieces, "mp", axis=0, tiled=True),
        down_weight.astype(jnp.float32).T,
        precision=lax.Precision.HIGHEST,
    )
    dp_count = lax.axis_size("dp")
    mp_count = lax.axis_size("mp")
    row_count = out_grad.shape[0]
    partial_value = partial_value.reshape(mp_count, dp_count * row_count, hid_units)
    summed = lax.psum_scatter(partial_value, "dp", scatter_dimension=1, tiled=True)
    return summed.reshape(mp_count * row_count, hid_units), gain_grad


def tile_of(hid):
    return next((t for t in (512, 256, 128) if hid % t == 0), 0)


def local(dp, mp, cotangent, mlp_out, post_gain, down_weight, gate_pre, up_pre):
    rows = cotangent.shape[0]
    hid, feat = down_weight.shape
    span = mp * rows
    held_bytes = span * hid * (2 * 12 + 4 + 12) + 4 * hid * feat + 20 * span * feat
    tiled = rows % 16 == 0 and tile_of(hid) > 0 and feat % LANES == 0
    paired = dp == 4 and mp % 4 == 0
    if tiled and paired and held_bytes < 60 * 1024 * 1024:
        return fused(dp, mp, cotangent, mlp_out, post_gain, down_weight, gate_pre, up_pre)
    hidden_grad, gain_grad = plain(cotangent, mlp_out, post_gain, down_weight)
    gate_val = gate_pre.astype(jnp.float32)
    up_val = up_pre.astype(jnp.float32)
    act_val, pull_back = jax.vjp(gelu_tanh, gate_val)
    gate_grad = pull_back(hidden_grad * up_val)[0]
    up_grad = hidden_grad * act_val
    return (gate_grad, up_grad, gain_grad)


def solution(mesh):
    return jax.shard_map(
        functools.partial(local, mesh.shape["dp"], mesh.shape["mp"]),
        mesh=mesh,
        in_specs=(
            P(("dp", "mp"), None),
            P(("dp", "mp"), None),
            P(),
            P("mp", "dp"),
            P("dp", "mp"),
            P("dp", "mp"),
        ),
        out_specs=(P("dp", "mp"), P("dp", "mp"), P()),
        check_vma=False,
    )
```
